512 devices in a mesh: zero: 32 (over y, x), width: 16 (over z, core).
Axes of the slice: x: 4, y: 8, z: 8, core: 2. Of those that a mesh axis runs over, the one named last changes fastest.
Arguments:
- w_gate: bfloat16 [3072, 8192], P('zero', 'width'), may hold values from -0.109375 to 0.109375
- low_gate: bfloat16 [3072, 16], P('zero'), may hold values from -0.109375 to 0.109375
- high_gate: bfloat16 [16, 8192], P(None, 'width'), may hold values from -1.5 to 1.5
- w_up: bfloat16 [3072, 8192], P('zero', 'width'), may hold values from -0.109375 to 0.109375
- low_up: bfloat16 [3072, 16], P('zero'), may hold values from -0.109375 to 0.109375
- high_up: bfloat16 [16, 8192], P(None, 'width'), may hold values from -1.5 to 1.5
- norm_train: float32 [3072], P(('zero', 'width')), may hold values from 0.25 to 1.75
- norm_step: float32 [3072], P(('zero', 'width')), may hold values from -0.3 to 0.3
Outputs:
- serving_gate: bfloat16 [8192, 3072], P('width')
- serving_up: bfloat16 [8192, 3072], P('width')
- serve_norm: bfloat16 [3072], replicated
The draws below stay inside these ranges and needn't reach their ends.
All inputs are finite; a program needn't handle non-finite values.
Results may differ from the reference program's by a relative error of at most 0.001.
Values may be sent and summed in bfloat16 or wider, within the bound.
No kernel may reach another device: no remote copies, remote signals or barrier semaphores. Data moves between devices by JAX's collectives and lax.ppermute only.
A program may use at most 64 MiB of HBM per device.

```python
import jax
import jax.numpy as jnp

D_MODEL = 3072
D_INNER = 8192
RANK = 16


def block_scale(own_key, shape, split, smallest, largest):
    level, own = 1.0, jax.random.fold_in(own_key, 6)
    for axis_at, parts in split:
        steps = jnp.exp(jax.random.uniform(jax.random.fold_in(own, axis_at), (parts,), jnp.float32, smallest / len(split), largest / len(split)))
        level = level * jnp.repeat(steps, shape[axis_at] // parts).reshape([-1 if axis == axis_at else 1 for axis in range(len(shape))])
    return level


def bell_draw(rng, shape, width, bound, shards=(), held_as=jnp.bfloat16):
    result = jax.random.normal(rng, shape, jnp.float32) * width
    if len(shards) > 0:
        result = block_scale(rng, shape, shards, -0.22, 0.18) * result
    return jnp.clip(result, min=-bound, max=bound).astype(held_as)


def setup_inputs(seed: int = 0) -> dict:
    streams_of = jax.random.split(jax.random.key(seed), 9)
    return {
        "w_gate": bell_draw(streams_of[0], (D_MODEL, D_INNER), D_MODEL ** -0.5, 0.109375, ((0, 32), (1, 16))),
        "low_gate": bell_draw(streams_of[1], (D_MODEL, RANK), D_MODEL ** -0.5, 0.109375, ((0, 32),)),
        "high_gate": bell_draw(streams_of[2], (RANK, D_INNER), RANK ** -0.5, 1.5, ((1, 16),)),
        "w_up": bell_draw(streams_of[3], (D_MODEL, D_INNER), D_MODEL ** -0.5, 0.109375, ((0, 32), (1, 16))),
        "low_up": bell_draw(streams_of[4], (D_MODEL, RANK), D_MODEL ** -0.5, 0.109375, ((0, 32),)),
        "high_up": bell_draw(streams_of[5], (RANK, D_INNER), RANK ** -0.5, 1.5, ((1, 16),)),
        "norm_train": jnp.clip(1.0 + 0.15 * jax.random.normal(streams_of[6], (D_MODEL,), jnp.float32), 0.25, 1.75),
        "norm_step": jnp.clip(jax.random.uniform(streams_of[7], (D_MODEL,), jnp.float32, -0.3, 0.3) * block_scale(streams_of[7], (D_MODEL,), ((0, 512),), -0.4, 0.0), -0.3, 0.3),
    }


mix_rate = 1.0


def reference(w_gate, low_gate, high_gate, w_up, low_up, high_up, norm_train, norm_step):
    whole_gate = w_gate.astype(jnp.float32) + mix_rate * jnp.dot(low_gate, high_gate, preferred_element_type=jnp.float32)
    whole_up = w_up.astype(jnp.float32) + mix_rate * jnp.dot(low_up, high_up, preferred_element_type=jnp.float32)
    serving_gate = whole_gate.T.astype(jnp.bfloat16)
    serving_up = whole_up.T.astype(jnp.bfloat16)
    serve_norm = (norm_train + norm_step).astype(jnp.bfloat16)
    return serving_gate, serving_up, serve_norm
```

```python
import jax
import jax.numpy as jnp
from jax import lax
from jax.experimental import pallas as pl
from jax.experimental.pallas import tpu as pltpu
from jax.sharding import PartitionSpec as P

mix_rate = 1.0
LANES, PIECE = 128, 96
NY, NX, NW = 8, 4, 16
N_FIRST = 5
N_LAST = 8 - N_FIRST
ROWS_FIRST = N_FIRST * PIECE + 8
ROWS_LAST = N_LAST * PIECE
X_ROWS = [[y * NX + x for x in range(NX)] for y in range(NY)]
Y_ROWS = [[y * NX + x for y in range(NY)] for x in range(NX)]


def swap(a, step):
    pairs = []
    for y in range(NY):
        for x in range(NX):
            d = 1 if (x + step) % 2 == 0 else -1
            pairs.append((y * NX + x, y * NX + (x + d) % NX))
    return lax.ppermute(a, "zero", pairs)


def merge_kernel(wg, lg, hg, wu, lu, hu, nt, ns, first, last):
    def whole(w, low_t, high):
        prod = lax.dot_general(low_t[...], high[...], (((0,), (0,)), ((), ())), preferred_element_type=jnp.float32)
        return (w[...].astype(jnp.float32) + mix_rate * prod).astype(jnp.bfloat16)

    gate, up = whole(wg, lg, hg), whole(wu, lu, hu)
    n = (nt[...] + ns[...]).astype(jnp.bfloat16)
    eye = (lax.broadcasted_iota(jnp.int32, (6, LANES), 0) == lax.broadcasted_iota(jnp.int32, (6, LANES), 1)).astype(jnp.bfloat16)
    rows = jnp.dot(jnp.broadcast_to(n, (8, 6)), eye, preferred_element_type=jnp.float32).astype(jnp.bfloat16)
    for t in range(8):
        c = (t % 4) * LANES
        tile = (gate if t < 4 else up)[:, c:c + LANES]
        if t < N_FIRST:
            for x in range(NX):
                first[x, t * PIECE:(t + 1) * PIECE, :] = tile
        else:
            last[(t - N_FIRST) * PIECE:(t - N_FIRST + 1) * PIECE, :] = tile
    for x in range(NX):
        first[x, N_FIRST * PIECE:, :] = rows


def last_kernel(pos, *refs):
    ins, (up, stage, blk, sem) = refs[:6], refs[6:]
    x, t = pos[0], pos[1]
    for h in range(2):
        own, near, far = ins[3 * h:3 * h + 3]
        s = t if h == 0 else -t
        at = [(x + m * s + 2 * NX) % NX for m in (0, 1, -1, -2)]

        @pl.loop(0, NY // 2)
        def _(g):
            for i in range(N_LAST):
                r = pl.ds(i * PIECE, PIECE)
                for k, part in enumerate((own[g, r, :], near[g, r, :], far[0, g, r, :], far[1, g, r, :])):
                    blk[i, pl.ds(pl.multiple_of(at[k] * PIECE, 32), PIECE), :] = part
            for i in range(N_LAST):
                stage[h * (NY // 2) + g, i * LANES:(i + 1) * LANES, :] = blk[i].T

    copies = [
        pltpu.make_async_copy(
            stage.at[y],
            up.at[pl.ds(512 - N_LAST * LANES, N_LAST * LANES), pl.ds(y * 384, 384)],
            sem.at[y],
        )
        for y in range(NY)
    ]
    for cp in copies:
        cp.start()
    for cp in copies:
        cp.wait()


def first_kernel(got, up_in, gate, up):
    for t in range(N_FIRST):
        block = jnp.concatenate([got[0, x, t * PIECE:(t + 1) * PIECE, :] for x in range(NX)], axis=0)
        out = gate if t < 4 else up
        out[(t % 4) * LANES:(t % 4 + 1) * LANES, :] = block.T


def norm_kernel(got, out):
    total = jnp.zeros((32, LANES), jnp.float32)
    e = lax.broadcasted_iota(jnp.int32, (LANES, LANES), 0)
    c = lax.broadcasted_iota(jnp.int32, (LANES, LANES), 1)
    for j in range(NW):
        pick = ((c == e + 6 * j) & (e < 6)).astype(jnp.bfloat16)
        total += jnp.dot(got[j], pick, preferred_element_type=jnp.float32)
    out[...] = total.astype(jnp.bfloat16)


def on_device(w_gate, low_gate, high_gate, w_up, low_up, high_up, norm_train, norm_step):
    vm = pl.BlockSpec(memory_space=pltpu.VMEM)
    sm = pl.BlockSpec(memory_space=pltpu.SMEM)
    hb = pl.BlockSpec(memory_space=pl.ANY)
    bf16 = jnp.bfloat16
    x = lax.axis_index("zero") & (NX - 1)
    pos = jnp.stack([x, 1 - 2 * (x & 1)]).astype(jnp.int32)
    first, last = pl.pallas_call(
        merge_kernel, in_specs=[vm] * 8, out_specs=[vm, vm],
        out_shape=[jax.ShapeDtypeStruct((NX, ROWS_FIRST, LANES), bf16), jax.ShapeDtypeStruct((ROWS_LAST, LANES), bf16)],
        name="merge",
    )(w_gate, low_gate.T, high_gate, w_up, low_up.T, high_up, norm_train[None, :], norm_step[None, :])

    along_x = lax.all_to_all(first, "zero", 0, 0, tiled=True, axis_index_groups=X_ROWS)
    got_first = lax.all_gather(along_x, "zero", axis=0, axis_index_groups=Y_ROWS)

    norm_x = along_x[:, N_FIRST * PIECE:, :].reshape(NX * 8, LANES)
    own = jnp.concatenate([last, norm_x], axis=0)
    along_y = lax.all_to_all(
        jnp.broadcast_to(own[None], (NY,) + own.shape), "zero", 0, 0, tiled=True, axis_index_groups=Y_ROWS)

    halves = []
    for h in range(2):
        a = along_y[h * 4:(h + 1) * 4, :ROWS_LAST]
        halves.append((a, swap(a, h)))
    norm_rows = along_y[:, ROWS_LAST:].reshape(32, 8, LANES)[:, 0, :]
    both = [jnp.stack(h) for h in halves]
    *both, norm_rows = lax.optimization_barrier((*both, norm_rows))
    parts = []
    for h in range(2):
        parts += [*halves[h], swap(both[h], 1 - h)]

    spread = lax.all_to_all(jnp.broadcast_to(norm_rows[None], (NW, 32, LANES)), "width", 0, 0, tiled=True)
    norm = pl.pallas_call(
        norm_kernel, in_specs=[vm], out_specs=vm, out_shape=jax.ShapeDtypeStruct((32, LANES), bf16), name="norm",
    )(spread)
    serve_norm = norm[:, :PIECE].reshape(3072)

    out = jax.ShapeDtypeStruct((512, 3072), bf16)
    up = pl.pallas_call(
        last_kernel, in_specs=[sm] + [vm] * 6, out_specs=hb, out_shape=out,
        scratch_shapes=[
            pltpu.VMEM((NY, N_LAST * LANES, 384), bf16),
            pltpu.VMEM((N_LAST, 384, LANES), bf16),
            pltpu.SemaphoreType.DMA((NY,)),
        ],
        name="last",
    )(pos, *parts)
    gate, up = pl.pallas_call(
        first_kernel, grid=(NY,),
        in_specs=[pl.BlockSpec((1, NX, ROWS_FIRST, LANES), lambda y: (y, 0, 0, 0)), hb],
        out_specs=[pl.BlockSpec((512, 384), lambda y: (0, y)), pl.BlockSpec(((N_FIRST - 4) * LANES, 384), lambda y: (0, y))],
        out_shape=[out, out], input_output_aliases={1: 1}, name="first",
    )(got_first, up)
    return (gate, up, serve_norm)


def solution(mesh):
    placed = (
        P("zero", "width"), P("zero", None), P(None, "width"),
        P("zero", "width"), P("zero", None), P(None, "width"),
        P(("zero", "width")), P(("zero", "width")),
    )
    return jax.shard_map(
        on_device, mesh=mesh, in_specs=placed,
        out_specs=(P("width", None), P("width", None), P()), check_vma=False,
    )
```

```python
import jax
import jax.numpy as jnp
from jax import lax
from jax.experimental import pallas as pl
from jax.experimental.pallas import tpu as pltpu
from jax.sharding import PartitionSpec as P

mix_rate = 1.0
LANES, PIECE = 128, 96
NY, NX, NW = 8, 4, 16
N_FIRST = 6
N_LAST = 8 - N_FIRST
ROWS_FIRST = N_FIRST * PIECE + 8
ROWS_LAST = N_LAST * PIECE
X_ROWS = [[y * NX + x for x in range(NX)] for y in range(NY)]
Y_ROWS = [[y * NX + x for y in range(NY)] for x in range(NX)]


def swap(a, step):
    pairs = []
    for y in range(NY):
        for x in range(NX):
            d = 1 if (x + step) % 2 == 0 else -1
            pairs.append((y * NX + x, y * NX + (x + d) % NX))
    return lax.ppermute(a, "zero", pairs)


def merge_kernel(pos, wg, lg, hg, wu, lu, hu, nt, ns, first, last):
    def whole(w, low_t, high):
        prod = lax.dot_general(low_t[...], high[...], (((0,), (0,)), ((), ())), preferred_element_type=jnp.float32)
        return (w[...].astype(jnp.float32) + mix_rate * prod).astype(jnp.bfloat16)

    gate, up = whole(wg, lg, hg), whole(wu, lu, hu)
    n = (nt[...] + ns[...]).astype(jnp.bfloat16)
    e = lax.broadcasted_iota(jnp.int32, (6, LANES), 0)
    eye = (e + pos[2] == lax.broadcasted_iota(jnp.int32, (6, LANES), 1)).astype(jnp.bfloat16)
    rows = jnp.dot(jnp.broadcast_to(n, (8, 6)), eye, preferred_element_type=jnp.float32).astype(jnp.bfloat16)
    for t in range(8):
        c = (t % 4) * LANES
        tile = (gate if t < 4 else up)[:, c:c + LANES]
        if t < N_FIRST:
            for x in range(NX):
                first[x, t * PIECE:(t + 1) * PIECE, :] = tile
        else:
            last[(t - N_FIRST) * PIECE:(t - N_FIRST + 1) * PIECE, :] = tile
    for x in range(NX):
        first[x, N_FIRST * PIECE:, :] = rows


def assemble(fetch, tiles, outs, buf, stage, sem_out):
    stores = []
    for y in range(NY):
        for cp in fetch[y]:
            cp.wait()
        for t in range(tiles):
            block = jnp.concatenate([buf[y, x, t * PIECE:(t + 1) * PIECE, :] for x in range(NX)], axis=0)
            stage[y, t * LANES:(t + 1) * LANES, :] = block.T
        for k, (out, at, row, rows) in enumerate(outs):
            cp = pltpu.make_async_copy(
                stage.at[y, pl.ds(at, rows), :], out.at[pl.ds(row, rows), pl.ds(y * 384, 384)], sem_out.at[k, y])
            cp.start()
            stores.append(cp)
    for cp in stores:
        cp.wait()


def last_kernel(pos, *refs):
    ins, (up, buf, stage, sem_in, sem_out) = refs[:6], refs[6:]
    fetch = []
    for y in range(NY):
        h, g = divmod(y, NY // 2)
        own, near, far = ins[3 * h:3 * h + 3]
        s = pos[1] if h == 0 else -pos[1]
        parts = ((own.at[g], 0), (near.at[g], 1), (far.at[0, g], -1), (far.at[1, g], -2))
        fetch.append([
            pltpu.make_async_copy(part, buf.at[y, (pos[0] + m * s + NX) & (NX - 1)], sem_in.at[y, k])
            for k, (part, m) in enumerate(parts)
        ])
        for cp in fetch[-1]:
            cp.start()
    n = N_LAST * LANES
    assemble(fetch, N_LAST, [(up, 0, 512 - n, n)], buf, stage, sem_out)


def first_kernel(got, up_in, gate, up, buf, stage, sem_in, sem_out):
    fetch = [[pltpu.make_async_copy(got.at[y], buf.at[y], sem_in.at[y])] for y in range(NY)]
    for cps in fetch:
        cps[0].start()
    n = (N_FIRST - 4) * LANES
    assemble(fetch, N_FIRST, [(gate, 0, 0, 512), (up, 512, 0, n)], buf, stage, sem_out)


def norm_kernel(got, out):
    total = jnp.zeros((32, LANES), jnp.float32)
    i = lax.broadcasted_iota(jnp.int32, (32, LANES), 0)
    lane = lax.broadcasted_iota(jnp.int32, (32, LANES), 1)
    at = lane - 6 * (i & 15)
    own = (at >= 0) & (at < 6)
    e = lax.broadcasted_iota(jnp.int32, (LANES, LANES), 0) % 6
    c = lax.broadcasted_iota(jnp.int32, (LANES, LANES), 1)
    for j in range(NW):
        r = got[j].astype(jnp.float32)
        rows = jnp.where(i < 16, jnp.broadcast_to(r[0:1], (32, LANES)), jnp.broadcast_to(r[1:2], (32, LANES)))
        rows = jnp.where(own, rows, 0.0).astype(jnp.bfloat16)
        total += jnp.dot(rows, (c == e + 6 * j).astype(jnp.bfloat16), preferred_element_type=jnp.float32)
    out[...] = total.astype(jnp.bfloat16)


def on_device(w_gate, low_gate, high_gate, w_up, low_up, high_up, norm_train, norm_step):
    vm = pl.BlockSpec(memory_space=pltpu.VMEM)
    sm = pl.BlockSpec(memory_space=pltpu.SMEM)
    hb = pl.BlockSpec(memory_space=pl.ANY)
    bf16 = jnp.bfloat16
    zero = lax.axis_index("zero")
    x = zero & (NX - 1)
    pos = jnp.stack([x, 1 - 2 * (x & 1), 6 * (zero & 15)]).astype(jnp.int32)
    first, last = pl.pallas_call(
        merge_kernel, in_specs=[sm] + [vm] * 8, out_specs=[vm, vm],
        out_shape=[jax.ShapeDtypeStruct((NX, ROWS_FIRST, LANES), bf16), jax.ShapeDtypeStruct((ROWS_LAST, LANES), bf16)],
        name="merge",
    )(pos, w_gate, low_gate.T, high_gate, w_up, low_up.T, high_up, norm_train[None, :], norm_step[None, :])

    along_x = lax.all_to_all(first, "zero", 0, 0, tiled=True, axis_index_groups=X_ROWS)
    got_first = lax.all_gather(along_x, "zero", axis=0, axis_index_groups=Y_ROWS)

    norm_x = jnp.sum(along_x[:, N_FIRST * PIECE:, :].astype(jnp.float32), axis=0).astype(bf16)
    own = jnp.concatenate([last, norm_x], axis=0)
    along_y = lax.all_to_all(
        jnp.broadcast_to(own[None], (NY,) + own.shape), "zero", 0, 0, tiled=True, axis_index_groups=Y_ROWS)

    halves = []
    for h in range(2):
        a = along_y[h * 4:(h + 1) * 4, :ROWS_LAST]
        halves.append((a, swap(a, h)))
    norm_y = along_y[:, ROWS_LAST:].astype(jnp.float32).reshape(2, 4, 8, LANES)
    norm_rows = jnp.sum(norm_y, axis=1)[:, 0, :]
    norm_rows = jnp.concatenate([norm_rows, jnp.zeros((6, LANES), jnp.float32)], axis=0).astype(bf16)
    both = [jnp.stack(h) for h in halves]
    *both, norm_rows = lax.optimization_barrier((*both, norm_rows))
    parts = []
    for h in range(2):
        parts += [*halves[h], swap(both[h], 1 - h)]

    spread = lax.all_to_all(jnp.broadcast_to(norm_rows[None], (NW, 8, LANES)), "width", 0, 0, tiled=True)
    norm = pl.pallas_call(
        norm_kernel, in_specs=[vm], out_specs=vm, out_shape=jax.ShapeDtypeStruct((32, LANES), bf16), name="norm",
    )(spread)
    serve_norm = norm[:, :PIECE].reshape(3072)

    out = jax.ShapeDtypeStruct((512, 3072), bf16)

    def scratch(rows, tiles, n_out, sem_in):
        return [
            pltpu.VMEM((NY, NX, rows, LANES), bf16),
            pltpu.VMEM((NY, tiles * LANES, 384), bf16),
            pltpu.SemaphoreType.DMA(sem_in),
            pltpu.SemaphoreType.DMA((n_out, NY)),
        ]

    up = pl.pallas_call(
        last_kernel, in_specs=[sm] + [hb] * 6, out_specs=hb, out_shape=out,
        scratch_shapes=scratch(ROWS_LAST, N_LAST, 1, (NY, NX)), name="last",
    )(pos, *parts)
    gate, up = pl.pallas_call(
        first_kernel, in_specs=[hb, hb], out_specs=[hb, hb], out_shape=[out, out],
        scratch_shapes=scratch(ROWS_FIRST, N_FIRST, 2, (NY,)), input_output_aliases={1: 1}, name="first",
    )(got_first, up)
    return (gate, up, serve_norm)


def solution(mesh):
    placed = (
        P("zero", "width"), P("zero", None), P(None, "width"),
        P("zero", "width"), P("zero", None), P(None, "width"),
        P(("zero", "width")), P(("zero", "width")),
    )
    return jax.shard_map(
        on_device, mesh=mesh, in_specs=placed,
        out_specs=(P("width", None), P("width", None), P()), check_vma=False,
    )
```

```python
import jax
import jax.numpy as jnp
from jax import lax
from jax.experimental import pallas as pl
from jax.experimental.pallas import tpu as pltpu
from jax.sharding import PartitionSpec as P


mix_rate = 1.0
LANES, PIECE = 128, 96
NY, NX, NW = 8, 4, 16
N_FIRST = 6
N_LAST = 8 - N_FIRST
ROWS_FIRST = N_FIRST * PIECE + 8
ROWS_LAST = N_LAST * PIECE
X_ROWS = [[y * NX + x for x in range(NX)] for y in range(NY)]
Y_ROWS = [[y * NX + x for y in range(NY)] for x in range(NX)]


def swap(a, step):
    pairs = []
    for y in range(NY):
        for x in range(NX):
            d = 1 if (x + step) % 2 == 0 else -1
            pairs.append((y * NX + x, y * NX + (x + d) % NX))
    return lax.ppermute(a, "zero", pairs)


def merge_kernel(wg, lg, hg, wu, lu, hu, nt, ns, first, last):
    def whole(w, low_t, high):
        prod = lax.dot_general(low_t[...], high[...], (((0,), (0,)), ((), ())), preferred_element_type=jnp.float32)
        return (w[...].astype(jnp.float32) + mix_rate * prod).astype(jnp.bfloat16)

    gate, up = whole(wg, lg, hg), whole(wu, lu, hu)
    at = 96 * (lax.axis_index("zero") & (NX - 1)) + 6 * lax.axis_index("width")
    n = jnp.broadcast_to((nt[...] + ns[...]).astype(jnp.bfloat16), (8, 6))
    e = lax.broadcasted_iota(jnp.int32, (6, LANES), 0)
    lane = lax.broadcasted_iota(jnp.int32, (6, LANES), 1)
    row = lax.broadcasted_iota(jnp.int32, (8, LANES), 0)
    rows = jnp.zeros((8, LANES), jnp.float32)
    for r in range(3):
        eye = (e + at == lane + r * LANES).astype(jnp.bfloat16)
        rows = jnp.where(row == r, jnp.dot(n, eye, preferred_element_type=jnp.float32), rows)
    rows = rows.astype(jnp.bfloat16)
    for t in range(8):
        c = (t % 4) * LANES
        tile = (gate if t < 4 else up)[:, c:c + LANES]
        if t < N_FIRST:
            for x in range(NX):
                first[x, t * PIECE:(t + 1) * PIECE, :] = tile
        else:
            last[(t - N_FIRST) * PIECE:(t - N_FIRST + 1) * PIECE, :] = tile
    for x in range(NX):
        first[x, N_FIRST * PIECE:, :] = rows


def assemble(fetch, tiles, outs, buf, stage, sem_out):
    stores = []
    for y in range(NY):
        for cp in fetch[y]:
            cp.wait()
        for t in range(tiles):
            block = jnp.concatenate([buf[y, x, t * PIECE:(t + 1) * PIECE, :] for x in range(NX)], axis=0)
            stage[y, t * LANES:(t + 1) * LANES, :] = block.T
        for k, (out, at, row, rows) in enumerate(outs):
            cp = pltpu.make_async_copy(
                stage.at[y, pl.ds(at, rows), :], out.at[pl.ds(row, rows), pl.ds(y * 384, 384)], sem_out.at[k, y])
            cp.start()
            stores.append(cp)
    for cp in stores:
        cp.wait()


def last_kernel(*refs):
    x = lax.axis_index("zero") & (NX - 1)
    ins, (up, buf, stage, sem_in, sem_out) = refs[:6], refs[6:]
    fetch = []
    for y in range(NY):
        h, g = divmod(y, NY // 2)
        own, near, far = ins[3 * h:3 * h + 3]
        s = (1 - 2 * (x & 1)) * (1 - 2 * h)
        parts = ((own.at[g], 0), (near.at[g], 1), (far.at[0, g], -1), (far.at[1, g], -2))
        fetch.append([
            pltpu.make_async_copy(part, buf.at[y, (x + m * s + NX) & (NX - 1)], sem_in.at[y, k])
            for k, (part, m) in enumerate(parts)
        ])
        for cp in fetch[-1]:
            cp.start()
    n = N_LAST * LANES
    assemble(fetch, N_LAST, [(up, 0, 512 - n, n)], buf, stage, sem_out)


def first_kernel(got, up_in, gate, up, buf, stage, sem_in, sem_out):
    fetch = [[pltpu.make_async_copy(got.at[y], buf.at[y], sem_in.at[y])] for y in range(NY)]
    for cps in fetch:
        cps[0].start()
    n = (N_FIRST - 4) * LANES
    assemble(fetch, N_FIRST, [(gate, 0, 0, 512), (up, 512, 0, n)], buf, stage, sem_out)


def program(w_gate, low_gate, high_gate, w_up, low_up, high_up, norm_train, norm_step):
    vm = pl.BlockSpec(memory_space=pltpu.VMEM)
    hb = pl.BlockSpec(memory_space=pl.ANY)
    bf16 = jnp.bfloat16
    first, last = pl.pallas_call(
        merge_kernel, in_specs=[vm] * 8, out_specs=[vm, vm],
        out_shape=[jax.ShapeDtypeStruct((NX, ROWS_FIRST, LANES), bf16), jax.ShapeDtypeStruct((ROWS_LAST, LANES), bf16)],
        name="merge",
    )(w_gate, low_gate.T, high_gate, w_up, low_up.T, high_up, norm_train[None, :], norm_step[None, :])

    along_x = lax.all_to_all(first, "zero", 0, 0, tiled=True, axis_index_groups=X_ROWS)
    got_first = lax.all_gather(along_x, "zero", axis=0, axis_index_groups=Y_ROWS)

    norm_x = jnp.sum(along_x[:, N_FIRST * PIECE:, :].astype(jnp.float32), axis=0).astype(bf16)
    own = jnp.concatenate([last, norm_x], axis=0)
    along_y = lax.all_to_all(
        jnp.broadcast_to(own[None], (NY,) + own.shape), "zero", 0, 0, tiled=True, axis_index_groups=Y_ROWS)

    norm_xy = along_y[:, ROWS_LAST:ROWS_LAST + 3].reshape(24, LANES)
    spread = lax.all_to_all(jnp.broadcast_to(norm_xy[None], (NW, 24, LANES)), "width", 0, 0, tiled=True)
    serve_norm = jnp.sum(spread.astype(jnp.float32), axis=0).astype(bf16).reshape(3072)

    halves = []
    for h in range(2):
        a = along_y[h * 4:(h + 1) * 4, :ROWS_LAST]
        halves.append((a, swap(a, h)))
    both = [jnp.concatenate([a[None], b[None]], axis=0) for a, b in halves]
    parts = []
    for h in range(2):
        parts += [*halves[h], swap(both[h], 1 - h)]

    out = jax.ShapeDtypeStruct((512, 3072), bf16)

    def scratch(rows, tiles, n_out, sem_in):
        return [
            pltpu.VMEM((NY, NX, rows, LANES), bf16),
            pltpu.VMEM((NY, tiles * LANES, 384), bf16),
            pltpu.SemaphoreType.DMA(sem_in),
            pltpu.SemaphoreType.DMA((n_out, NY)),
        ]

    up = pl.pallas_call(
        last_kernel, in_specs=[hb] * 6, out_specs=hb, out_shape=out,
        scratch_shapes=scratch(ROWS_LAST, N_LAST, 1, (NY, NX)), name="last",
    )(*parts)
    gate, up = pl.pallas_call(
        first_kernel, in_specs=[hb, hb], out_specs=[hb, hb], out_shape=[out, out],
        scratch_shapes=scratch(ROWS_FIRST, N_FIRST, 2, (NY,)), input_output_aliases={1: 1}, name="first",
    )(got_first, up)
    return (gate, up, serve_norm)


def solution(mesh):
    placed = (
        P("zero", "width"), P("zero", None), P(None, "width"),
        P("zero", "width"), P("zero", None), P(None, "width"),
        P(("zero", "width")), P(("zero", "width")),
    )
    return jax.shard_map(
        program, mesh=mesh, in_specs=placed,
        out_specs=(P("width", None), P("width", None), P()), check_vma=False,
    )
```

```python
import jax
import jax.numpy as jnp
from jax import lax
from jax.experimental import pallas as pl
from jax.experimental.pallas import tpu as pltpu
from jax.sharding import PartitionSpec as P


mix_rate = 1.0
LANES, PIECE = 128, 96
NY, NX, NW = 8, 4, 16
N_FIRST = 5
N_LAST = 8 - N_FIRST
ROWS_FIRST = N_FIRST * PIECE + 8
ROWS_LAST = N_LAST * PIECE
X_ROWS = [[y * NX + x for x in range(NX)] for y in range(NY)]
Y_ROWS = [[y * NX + x for y in range(NY)] for x in range(NX)]


def swap(a, step):
    pairs = []
    for y in range(NY):
        for x in range(NX):
            d = 1 if (x + step) % 2 == 0 else -1
            pairs.append((y * NX + x, y * NX + (x + d) % NX))
    return lax.ppermute(a, "zero", pairs)


def merge_kernel(wg, lg, hg, wu, lu, hu, nt, ns, first, last):
    def whole(w, low_t, high):
        prod = lax.dot_general(low_t[...], high[...], (((0,), (0,)), ((), ())), preferred_element_type=jnp.float32)
        return (w[...].astype(jnp.float32) + mix_rate * prod).astype(jnp.bfloat16)

    gate, up = whole(wg, lg, hg), whole(wu, lu, hu)
    at = 96 * (lax.axis_index("zero") & (NX - 1)) + 6 * lax.axis_index("width")
    n = jnp.broadcast_to((nt[...] + ns[...]).astype(jnp.bfloat16), (8, 6))
    e = lax.broadcasted_iota(jnp.int32, (6, LANES), 0)
    lane = lax.broadcasted_iota(jnp.int32, (6, LANES), 1)
    row = lax.broadcasted_iota(jnp.int32, (8, LANES), 0)
    rows = jnp.zeros((8, LANES), jnp.float32)
    for r in range(3):
        eye = (e + at == lane + r * LANES).astype(jnp.bfloat16)
        rows = jnp.where(row == r, jnp.dot(n, eye, preferred_element_type=jnp.float32), rows)
    rows = rows.astype(jnp.bfloat16)
    for t in range(8):
        c = (t % 4) * LANES
        tile = (gate if t < 4 else up)[:, c:c + LANES]
        if t < N_FIRST:
            for x in range(NX):
                first[x, t * PIECE:(t + 1) * PIECE, :] = tile
        else:
            last[(t - N_FIRST) * PIECE:(t - N_FIRST + 1) * PIECE, :] = tile
    for x in range(NX):
        first[x, N_FIRST * PIECE:, :] = rows


def assemble(fetch, tiles, outs, buf, stage, sem_out):
    stores = []
    for y in range(NY):
        for cp in fetch[y]:
            cp.wait()
        for t in range(tiles):
            block = jnp.concatenate([buf[y, x, t * PIECE:(t + 1) * PIECE, :] for x in range(NX)], axis=0)
            stage[y, t * LANES:(t + 1) * LANES, :] = block.T
        for k, (out, at, row, rows) in enumerate(outs):
            cp = pltpu.make_async_copy(
                stage.at[y, pl.ds(at, rows), :], out.at[pl.ds(row, rows), pl.ds(y * 384, 384)], sem_out.at[k, y])
            cp.start()
            stores.append(cp)
    return stores


def fetch_last(ins, buf, sem_in):
    x = lax.axis_index("zero") & (NX - 1)
    fetch = []
    for y in range(NY):
        h, g = divmod(y, NY // 2)
        own, near, far = ins[3 * h:3 * h + 3]
        s = (1 - 2 * (x & 1)) * (1 - 2 * h)
        parts = ((own.at[g], 0), (near.at[g], 1), (far.at[0, g], -1), (far.at[1, g], -2))
        fetch.append([
            pltpu.make_async_copy(part, buf.at[y, (x + m * s + NX) & (NX - 1)], sem_in.at[y, k])
            for k, (part, m) in enumerate(parts)
        ])
        for cp in fetch[-1]:
            cp.start()
    return fetch


def place_kernel(got, *refs):
    parts, (gate, up, buf, stage, sem_in, sem_out, buf_l, stage_l, sem_in_l, sem_out_l) = refs[:6], refs[6:]
    fetch = [[pltpu.make_async_copy(got.at[y], buf.at[y], sem_in.at[y])] for y in range(NY)]
    for cps in fetch:
        cps[0].start()
    late = fetch_last(parts, buf_l, sem_in_l)
    n, m = (N_FIRST - 4) * LANES, N_LAST * LANES
    stores = assemble(fetch, N_FIRST, [(gate, 0, 0, 512), (up, 512, 0, n)], buf, stage, sem_out)
    stores += assemble(late, N_LAST, [(up, 0, 512 - m, m)], buf_l, stage_l, sem_out_l)
    for cp in stores:
        cp.wait()


def program(w_gate, low_gate, high_gate, w_up, low_up, high_up, norm_train, norm_step):
    vm = pl.BlockSpec(memory_space=pltpu.VMEM)
    hb = pl.BlockSpec(memory_space=pl.ANY)
    bf16 = jnp.bfloat16
    first, last = pl.pallas_call(
        merge_kernel, in_specs=[vm] * 8, out_specs=[vm, vm],
        out_shape=[jax.ShapeDtypeStruct((NX, ROWS_FIRST, LANES), bf16), jax.ShapeDtypeStruct((ROWS_LAST, LANES), bf16)],
        name="merge",
    )(w_gate, low_gate.T, high_gate, w_up, low_up.T, high_up, norm_train[None, :], norm_step[None, :])

    along_x = lax.all_to_all(first, "zero", 0, 0, tiled=True, axis_index_groups=X_ROWS)
    got_first = lax.all_gather(along_x, "zero", axis=0, axis_index_groups=Y_ROWS)

    norm_x = jnp.sum(along_x[:, N_FIRST * PIECE:, :].astype(jnp.float32), axis=0).astype(bf16)
    own = jnp.concatenate([last, norm_x], axis=0)
    along_y = lax.all_to_all(
        jnp.broadcast_to(own[None], (NY,) + own.shape), "zero", 0, 0, tiled=True, axis_index_groups=Y_ROWS)

    norm_xy = along_y[:, ROWS_LAST:ROWS_LAST + 3].reshape(24, LANES)
    norm_xy = norm_xy + lax.ppermute(norm_xy, "width", [(w, w ^ 1) for w in range(NW)])
    spread = lax.all_to_all(
        jnp.broadcast_to(norm_xy[None], (NW // 2, 24, LANES)), "width", 0, 0, tiled=True,
        axis_index_groups=[[2 * z + core for z in range(NW // 2)] for core in range(2)])
    serve_norm = jnp.sum(spread.astype(jnp.float32), axis=0).astype(bf16).reshape(3072)

    halves = []
    for h in range(2):
        a = along_y[h * 4:(h + 1) * 4, :ROWS_LAST]
        halves.append((a, swap(a, h)))
    near = lax.optimization_barrier(tuple(b for _, b in halves))
    halves = [(a, b) for (a, _), b in zip(halves, near)]
    both = [jnp.concatenate([a[None], b[None]], axis=0) for a, b in halves]
    parts = []
    for h in range(2):
        parts += [*halves[h], swap(both[h], 1 - h)]

    out = jax.ShapeDtypeStruct((512, 3072), bf16)

    def scratch(rows, tiles, n_out, sem_in):
        return [
            pltpu.VMEM((NY, NX, rows, LANES), bf16),
            pltpu.VMEM((NY, tiles * LANES, 384), bf16),
            pltpu.SemaphoreType.DMA(sem_in),
            pltpu.SemaphoreType.DMA((n_out, NY)),
        ]

    gate, up = pl.pallas_call(
        place_kernel, in_specs=[hb] * 7, out_specs=[hb, hb], out_shape=[out, out],
        scratch_shapes=scratch(ROWS_FIRST, N_FIRST, 2, (NY,)) + scratch(ROWS_LAST, N_LAST, 1, (NY, NX)), name="place",
    )(got_first, *parts)
    return (gate, up, serve_norm)


def solution(mesh):
    placed = (
        P("zero", "width"), P("zero", None), P(None, "width"),
        P("zero", "width"), P("zero", None), P(None, "width"),
        P(("zero", "width")), P(("zero", "width")),
    )
    return jax.shard_map(
        program, mesh=mesh, in_specs=placed,
        out_specs=(P("width", None), P("width", None), P()), check_vma=False,
    )
```

```python
import jax
import jax.numpy as jnp
from jax import lax
from jax.experimental import pallas as pl
from jax.experimental.pallas import tpu as pltpu
from jax.sharding import PartitionSpec as P


mix_rate = 1.0
LANES, PIECE = 128, 96
NY, NX, NW = 8, 4, 16
N_FIRST = 5
N_LAST = 8 - N_FIRST
ROWS_FIRST = N_FIRST * PIECE + 8
ROWS_LAST = N_LAST * PIECE
X_ROWS = [[y * NX + x for x in range(NX)] for y in range(NY)]
Y_ROWS = [[y * NX + x for y in range(NY)] for x in range(NX)]


def swap(a, step):
    pairs = []
    for y in range(NY):
        for x in range(NX):
            d = 1 if (x + step) % 2 == 0 else -1
            pairs.append((y * NX + x, y * NX + (x + d) % NX))
    return lax.ppermute(a, "zero", pairs)


def merge_kernel(wg, lg, hg, wu, lu, hu, nt, ns, first, last):
    def whole(w, low_t, high):
        prod = lax.dot_general(low_t[...], high[...], (((0,), (0,)), ((), ())), preferred_element_type=jnp.float32)
        return (w[...].astype(jnp.float32) + mix_rate * prod).astype(jnp.bfloat16)

    gate, up = whole(wg, lg, hg), whole(wu, lu, hu)
    at = 96 * (lax.axis_index("zero") & (NX - 1)) + 6 * lax.axis_index("width")
    n = jnp.broadcast_to((nt[...] + ns[...]).astype(jnp.bfloat16), (8, 6))
    e = lax.broadcasted_iota(jnp.int32, (6, LANES), 0)
    lane = lax.broadcasted_iota(jnp.int32, (6, LANES), 1)
    row = lax.broadcasted_iota(jnp.int32, (8, LANES), 0)
    rows = jnp.zeros((8, LANES), jnp.float32)
    for r in range(3):
        eye = (e + at == lane + r * LANES).astype(jnp.bfloat16)
        rows = jnp.where(row == r, jnp.dot(n, eye, preferred_element_type=jnp.float32), rows)
    rows = rows.astype(jnp.bfloat16)
    for t in range(8):
        c = (t % 4) * LANES
        tile = (gate if t < 4 else up)[:, c:c + LANES]
        if t < N_FIRST:
            for x in range(NX):
                first[x, t * PIECE:(t + 1) * PIECE, :] = tile
        else:
            for y in range(NY):
                last[y, (t - N_FIRST) * PIECE:(t - N_FIRST + 1) * PIECE, :] = tile
    for x in range(NX):
        first[x, N_FIRST * PIECE:, :] = rows
    for y in range(NY):
        last[y, ROWS_LAST:, :] = jnp.zeros((8, LANES), jnp.bfloat16)


def assemble(fetch, tiles, outs, buf, stage, sem_out):
    stores = []
    for y in range(NY):
        for cp in fetch[y]:
            cp.wait()
        for t in range(tiles):
            block = jnp.concatenate([buf[y, x, t * PIECE:(t + 1) * PIECE, :] for x in range(NX)], axis=0)
            stage[y, t * LANES:(t + 1) * LANES, :] = block.T
        for k, (out, at, row, rows) in enumerate(outs):
            cp = pltpu.make_async_copy(
                stage.at[y, pl.ds(at, rows), :], out.at[pl.ds(row, rows), pl.ds(y * 384, 384)], sem_out.at[k, y])
            cp.start()
            stores.append(cp)
    return stores


def fetch_last(ins, buf, sem_in):
    x = lax.axis_index("zero") & (NX - 1)
    fetch = []
    for y in range(NY):
        h, g = divmod(y, NY // 2)
        own, near, far = ins[3 * h:3 * h + 3]
        s = (1 - 2 * (x & 1)) * (1 - 2 * h)
        parts = ((own.at[g], 0), (near.at[g], 1), (far.at[0, g], -1), (far.at[1, g], -2))
        fetch.append([
            pltpu.make_async_copy(part, buf.at[y, (x + m * s + NX) & (NX - 1)], sem_in.at[y, k])
            for k, (part, m) in enumerate(parts)
        ])
        for cp in fetch[-1]:
            cp.start()
    return fetch


def place_kernel(got, *refs):
    parts, (gate, up, buf, stage, sem_in, sem_out, buf_l, stage_l, sem_in_l, sem_out_l) = refs[:6], refs[6:]
    fetch = [[pltpu.make_async_copy(got.at[y], buf.at[y], sem_in.at[y])] for y in range(NY)]
    for cps in fetch:
        cps[0].start()
    late = fetch_last(parts, buf_l, sem_in_l)
    n, m = (N_FIRST - 4) * LANES, N_LAST * LANES
    stores = assemble(fetch, N_FIRST, [(gate, 0, 0, 512), (up, 512, 0, n)], buf, stage, sem_out)
    stores += assemble(late, N_LAST, [(up, 0, 512 - m, m)], buf_l, stage_l, sem_out_l)
    for cp in stores:
        cp.wait()


def program(w_gate, low_gate, high_gate, w_up, low_up, high_up, norm_train, norm_step):
    vm = pl.BlockSpec(memory_space=pltpu.VMEM)
    hb = pl.BlockSpec(memory_space=pl.ANY)
    bf16 = jnp.bfloat16
    first, last = pl.pallas_call(
        merge_kernel, in_specs=[vm] * 8, out_specs=[vm, vm],
        out_shape=[jax.ShapeDtypeStruct((NX, ROWS_FIRST, LANES), bf16), jax.ShapeDtypeStruct((NY, ROWS_LAST + 8, LANES), bf16)],
        name="merge",
    )(w_gate, low_gate.T, high_gate, w_up, low_up.T, high_up, norm_train[None, :], norm_step[None, :])

    along_x = lax.all_to_all(first, "zero", 0, 0, tiled=True, axis_index_groups=X_ROWS)
    got_first = lax.all_gather(along_x, "zero", axis=0, axis_index_groups=Y_ROWS)

    norm_x = jnp.sum(along_x[:, N_FIRST * PIECE:, :].astype(jnp.float32), axis=0).astype(bf16)
    own = lax.dynamic_update_slice(last, jnp.broadcast_to(norm_x[None], (NY, 8, LANES)), (0, ROWS_LAST, 0))
    along_y = lax.all_to_all(own, "zero", 0, 0, tiled=True, axis_index_groups=Y_ROWS)

    norm_xy = along_y[:, ROWS_LAST:ROWS_LAST + 3].reshape(24, LANES)
    norm_xy = norm_xy + lax.ppermute(norm_xy, "width", [(w, w ^ 1) for w in range(NW)])
    spread = lax.all_to_all(
        jnp.broadcast_to(norm_xy[None], (NW // 2, 24, LANES)), "width", 0, 0, tiled=True,
        axis_index_groups=[[2 * z + core for z in range(NW // 2)] for core in range(2)])
    serve_norm = jnp.sum(spread.astype(jnp.float32), axis=0).astype(bf16).reshape(3072)

    halves = []
    for h in range(2):
        a = along_y[h * 4:(h + 1) * 4, :ROWS_LAST]
        halves.append((a, swap(a, h)))
    near = lax.optimization_barrier(tuple(b for _, b in halves))
    halves = [(a, b) for (a, _), b in zip(halves, near)]
    both = [jnp.concatenate([a[None], b[None]], axis=0) for a, b in halves]
    parts = []
    for h in range(2):
        parts += [*halves[h], swap(both[h], 1 - h)]

    out = jax.ShapeDtypeStruct((512, 3072), bf16)

    def scratch(rows, tiles, n_out, sem_in):
        return [
            pltpu.VMEM((NY, NX, rows, LANES), bf16),
            pltpu.VMEM((NY, tiles * LANES, 384), bf16),
            pltpu.SemaphoreType.DMA(sem_in),
            pltpu.SemaphoreType.DMA((n_out, NY)),
        ]

    gate, up = pl.pallas_call(
        place_kernel, in_specs=[hb] * 7, out_specs=[hb, hb], out_shape=[out, out],
        scratch_shapes=scratch(ROWS_FIRST, N_FIRST, 2, (NY,)) + scratch(ROWS_LAST, N_LAST, 1, (NY, NX)), name="place",
    )(got_first, *parts)
    return (gate, up, serve_norm)


def solution(mesh):
    placed = (
        P("zero", "width"), P("zero", None), P(None, "width"),
        P("zero", "width"), P("zero", None), P(None, "width"),
        P(("zero", "width")), P(("zero", "width")),
    )
    return jax.shard_map(
        program, mesh=mesh, in_specs=placed,
        out_specs=(P("width", None), P("width", None), P()), check_vma=False,
    )
```
